32 devices in a mesh: space: 8 (over z, y), tm: 4 (over x, core).
Axes of the slice: x: 2, y: 2, z: 4, core: 2. Of those that a mesh axis runs over, the one named last changes fastest.
Arguments:
- innovations: bfloat16 [12, 32, 768, 1536], P('tm', None, 'space'), may hold values from -6 to 6
- obs_counts: int32 [12, 192, 384], P('tm', 'space'), may hold values from 0 to 3
- diffusion: float32 [32, 192, 384], P(None, 'space'), may hold values from 0.01 to 0.1
- courant: float32 [32, 192, 384], P(None, 'space'), may hold values from 0 to 0.4
Outputs:
- increment: float32 [32, 768, 1536], P('tm', 'space')
- residual: float32 [32, 192, 384], P('tm', 'space')
The draws below stay inside these ranges and needn't reach their ends.
All inputs are finite; a program needn't handle non-finite values.
Results may differ from the reference program's by a relative error of at most 0.0003.
Values sent between devices are 32-bit elements; how exact they have to be, the bound alone decides.
A program may use at most 384 MiB of HBM per device.

```python
import math
import jax
import jax.numpy as jnp
from jax import lax

NLAT_F = 768
NLON_F = 1536
LEV = 32
ITERS = 3
NLAT = 192
NLON = 384
STEPS = 12


def touch_ends(entries, rng, smallest, high):
    spot = [jax.random.randint(jax.random.fold_in(rng, axis), (), 0, length) for axis, length in enumerate(entries.shape)]
    main_axis = entries.shape.index(max(entries.shape))
    next_to = spot[:main_axis] + [(spot[main_axis] + 1) % entries.shape[main_axis]] + spot[main_axis + 1:]
    return entries.at[tuple(spot)].set(smallest).at[tuple(next_to)].set(high)


def levels(rng, dims, split, smallest, high):
    factor_of, own = 1.0, jax.random.fold_in(rng, 6)
    for axis_at, parts in split:
        draws = jnp.exp(jax.random.uniform(jax.random.fold_in(own, axis_at), (parts,), jnp.float32, smallest / len(split), high / len(split)))
        factor_of = factor_of * jnp.repeat(draws, dims[axis_at] // parts).reshape([-1 if axis == axis_at else 1 for axis in range(len(dims))])
    return factor_of


def bell_draw(key, shape, spread, limit, cuts=(), held_as=jnp.bfloat16):
    entries = spread * jax.random.normal(key, shape, jnp.float32)
    if cuts:
        entries = entries * levels(key, shape, cuts, -0.22, 0.18)
    return jnp.clip(entries, -limit, limit).astype(held_as)


def setup_inputs(seed: int = 0) -> dict:
    key_list = jax.random.split(jax.random.key(seed), 5)
    innovations = bell_draw(key_list[0], (STEPS, LEV, NLAT_F, NLON_F), 1.0, 6.0, ((0, 4), (2, 8)))
    obs_counts = touch_ends(jax.random.randint(key_list[1], (STEPS, NLAT, NLON), 0, 4), jax.random.fold_in(key_list[1], 1), 0, 3).astype(jnp.int32)
    diffusion = jnp.clip(jnp.exp(math.log(0.1) - 2.3025851 * jax.random.uniform(key_list[2], (LEV, NLAT, NLON), jnp.float32) ** levels(key_list[2], (LEV, NLAT, NLON), ((1, 8),), -0.2, 0.2)), 0.01, 0.1)
    courant = jnp.clip(0.4 * jax.random.uniform(key_list[3], (LEV, NLAT, NLON), jnp.float32) ** levels(key_list[3], (LEV, NLAT, NLON), ((1, 8),), -0.2, 0.2), 0.0, 0.4)
    return {"innovations": innovations, "obs_counts": obs_counts, "diffusion": diffusion, "courant": courant}


def laplace(state_field):
    padded = jnp.pad(state_field, ((0, 0), (1, 1), (0, 0)))
    return padded[:, 2:, :] + padded[:, :-2, :] + jnp.roll(state_field, 1, 2) + jnp.roll(state_field, -1, 2) - 4.0 * state_field


def tangent(state_field, diffusion, courant):
    return state_field + diffusion * laplace(state_field) - courant * (state_field - jnp.roll(state_field, 1, 2))


def adjoint(state_field, diffusion, courant):
    carried = courant * state_field
    return state_field + laplace(diffusion * state_field) - carried + jnp.roll(carried, -1, 2)


def restrict(block_field):
    coarse = block_field.astype(jnp.float32).reshape(LEV, NLAT_F // 4, 4, NLON_F // 4, 4)
    return jnp.mean(coarse, axis=(2, 4))


def reference(innovations, obs_counts, diffusion, courant):
    weights = obs_counts.astype(jnp.float32)[:, None]
    forcing = weights * lax.map(restrict, innovations)

    def forward(state_field):
        records = []
        for step_no in range(STEPS):
            records.append(weights[step_no] * state_field)
            if step_no + 1 < STEPS:
                state_field = tangent(state_field, diffusion, courant)
        return jnp.stack(records)

    def backward(terms):
        current = terms[STEPS - 1]
        for step_no in range(STEPS - 2, -1, -1):
            current = terms[step_no] + adjoint(current, diffusion, courant)
        return current

    rhs_field = backward(forcing)
    control = jnp.zeros_like(rhs_field)
    residual = rhs_field
    direction = rhs_field
    norm_now = jnp.sum(residual * residual)
    for iter_no in range(ITERS):
        hessian_image = direction + backward(forward(direction))
        step_len = norm_now / jnp.sum(direction * hessian_image)
        control = control + step_len * direction
        residual = residual - step_len * hessian_image
        if iter_no + 1 < ITERS:
            norm_next = jnp.sum(residual * residual)
            direction = residual + (norm_next / norm_now) * direction
            norm_now = norm_next
    increment = jnp.repeat(jnp.repeat(control, 4, axis=1), 4, axis=2)
    return increment, residual
```

```python
import functools

import jax
import jax.numpy as jnp
from jax import lax
from jax.experimental import pallas as pl
from jax.experimental.pallas import tpu as pltpu
from jax.sharding import PartitionSpec as P

ITERS = 3
F32 = jnp.float32
BF16 = jnp.bfloat16
MESH = pl.DeviceIdType.MESH
BLOCK = 4
COARSE = 4


def restrict_kernel(inn, counts, diff, cour, forcing, weights, diff_t, cour_t, summed):
    levels, fine_rows, fine_cols = inn.shape[1:]
    rows, cols = fine_rows // COARSE, fine_cols // COARSE
    weights[0] = counts[0].astype(F32)
    wide = 128 * COARSE
    pick = jnp.where(
        lax.broadcasted_iota(jnp.int32, (wide, 128), 0) // COARSE
        == lax.broadcasted_iota(jnp.int32, (wide, 128), 1),
        1.0 / (COARSE * COARSE),
        0.0,
    ).astype(BF16)
    for part in range(cols // 128):
        block = inn[0, :, :, part * wide : (part + 1) * wide].reshape(levels * fine_rows, wide)
        summed[part] = jnp.dot(block, pick, preferred_element_type=F32)
    for row in range(rows):
        for part in range(cols // 128):
            total = summed[part, pl.ds(COARSE * row, levels, stride=fine_rows), :]
            for sub in range(1, COARSE):
                total += summed[part, pl.ds(COARSE * row + sub, levels, stride=fine_rows), :]
            at = slice(part * 128, (part + 1) * 128)
            forcing[0, 0, row, :, at] = total * weights[0, row : row + 1, at]

    @pl.when(pl.program_id(1) == 0)
    def _():
        for row in range(rows):
            diff_t[0, row] = diff[:, row, :]
            cour_t[0, row] = cour[:, row, :]


def restrict_call(innovations, obs_counts, diffusion, courant, sections):
    steps, levels, fine_rows, fine_cols = innovations.shape
    part = levels // sections
    rows, cols = fine_rows // COARSE, fine_cols // COARSE
    field = pl.BlockSpec((part, rows, cols), lambda g, t: (g, 0, 0))
    field_t = pl.BlockSpec((1, rows, part, cols), lambda g, t: (g, 0, 0, 0))
    step = pl.BlockSpec((1, rows, cols), lambda g, t: (t, 0, 0))
    return pl.pallas_call(
        restrict_kernel,
        grid=(sections, steps),
        in_specs=[
            pl.BlockSpec((1, part, fine_rows, fine_cols), lambda g, t: (t, g, 0, 0)),
            step,
            field,
            field,
        ],
        out_specs=[
            pl.BlockSpec((1, 1, rows, part, cols), lambda g, t: (g, t, 0, 0, 0)),
            step,
            field_t,
            field_t,
        ],
        out_shape=[
            jax.ShapeDtypeStruct((sections, steps, rows, part, cols), F32),
            jax.ShapeDtypeStruct((steps, rows, cols), F32),
            jax.ShapeDtypeStruct((sections, rows, part, cols), F32),
            jax.ShapeDtypeStruct((sections, rows, part, cols), F32),
        ],
        scratch_shapes=[pltpu.VMEM((cols // 128, part * fine_rows, 128), F32)],
        compiler_params=pltpu.CompilerParams(vmem_limit_bytes=48 * 2**20),
        name="restrict",
    )(innovations, obs_counts, diffusion, courant)


def expand_kernel(control, residual, increment, residual_out, held, repeated):
    rows, cols = residual_out.shape[1:]
    part = control.shape[0] // rows
    level = pl.program_id(0)
    wide = 128 * COARSE

    @pl.when(level == 0)
    def _():
        for piece in range(cols // 128):
            held[0, piece] = control[:, piece * 128 : (piece + 1) * 128]
            held[1, piece] = residual[:, piece * 128 : (piece + 1) * 128]

    pick = jnp.where(
        lax.broadcasted_iota(jnp.int32, (128, wide), 1) // COARSE
        == lax.broadcasted_iota(jnp.int32, (128, wide), 0),
        1.0,
        0.0,
    ).astype(BF16)
    for piece in range(cols // 128):
        at = pl.ds(level, rows, stride=part)
        residual_out[0, :, piece * 128 : (piece + 1) * 128] = held[1, piece, at, :]
        values = held[0, piece, at, :]
        for sub in range(COARSE):
            repeated[piece, pl.ds(sub, rows, stride=COARSE), :] = values
        rest = repeated[piece]
        total = None
        for _ in range(3):
            head = rest.astype(BF16)
            rest = rest - head.astype(F32)
            spread = jnp.dot(head, pick, preferred_element_type=F32)
            total = spread if total is None else total + spread
        increment[0, :, piece * wide : (piece + 1) * wide] = total


def expand_call(control, residual):
    rows, part, cols = control.shape
    whole = pl.BlockSpec((rows * part, cols), lambda l: (0, 0))
    return pl.pallas_call(
        expand_kernel,
        grid=(part,),
        in_specs=[whole, whole],
        out_specs=[
            pl.BlockSpec((1, rows * COARSE, cols * COARSE), lambda l: (l, 0, 0)),
            pl.BlockSpec((1, rows, cols), lambda l: (l, 0, 0)),
        ],
        out_shape=[
            jax.ShapeDtypeStruct((part, rows * COARSE, cols * COARSE), F32),
            jax.ShapeDtypeStruct((part, rows, cols), F32),
        ],
        scratch_shapes=[
            pltpu.VMEM((2, cols // 128, rows * part, 128), F32),
            pltpu.VMEM((cols // 128, rows * COARSE, 128), F32),
        ],
        compiler_params=pltpu.CompilerParams(vmem_limit_bytes=32 * 2**20),
        name="expand",
    )(control.reshape(rows * part, cols), residual.reshape(rows * part, cols))


def solve_kernel(
    n_space,
    n_tm,
    forcing,
    weights,
    diff,
    cour,
    control,
    residual,
    co_a,
    co_b,
    co_d,
    states,
    wts,
    lam,
    direction,
    p_send,
    p_recv,
    w_recv,
    edge_recv,
    halo_recv,
    send_buf,
    swap_recv,
    red_src,
    red_tm,
    red_space,
    p_sems,
    w_sems,
    edge_sems,
    halo_sems,
    swap_sems,
    red_tm_sems,
    red_space_sems,
):
    steps, rows, part, cols = forcing.shape[1:]
    total_steps = steps * n_tm
    halo = total_steps - 1
    pad = halo + 1
    place = lax.axis_index("space")
    section = lax.axis_index("tm")
    above, below = place - 1, place + 1
    has_above, has_below = place > 0, place < n_space - 1
    own = pl.ds(pad, rows)
    top, bottom = pl.ds(pad - halo, halo), pl.ds(pad + rows, halo)

    def over_rows(low, count, fn):
        blocks = (count + BLOCK - 1) // BLOCK

        def one(block, carry):
            fn(low + block * BLOCK)
            return carry

        lax.fori_loop(0, blocks, one, 0)

    def clear(ref, count):
        def one(row, carry):
            ref[row] = jnp.zeros(ref.shape[1:], F32)
            return carry

        lax.fori_loop(0, count, one, 0)

    def to(axis, peer):
        return {"device_id": {axis: peer}, "device_id_type": MESH}

    edge_recv[...] = jnp.zeros_like(edge_recv)
    for side in range(2):
        for k in range(2):
            clear(halo_recv.at[side, k], halo)
        for k in range(swap_recv.shape[0]):
            clear(swap_recv.at[k, side], halo)

    tm_peers = [lax.rem(section + k, n_tm) for k in range(1, n_tm)]
    space_peers = [lax.rem(place + k, n_space) for k in range(1, n_space)]
    barrier = pltpu.get_barrier_semaphore()
    for peer in tm_peers:
        pl.semaphore_signal(barrier, inc=1, **to("tm", peer))
    for peer in space_peers:
        pl.semaphore_signal(barrier, inc=1, **to("space", peer))
    pl.semaphore_wait(barrier, n_tm - 1 + n_space - 1)

    def pair(up_src, down_src, up_dst, down_dst, sems):
        up = pltpu.make_async_remote_copy(
            src_ref=up_src, dst_ref=up_dst, send_sem=sems.at[0, 0], recv_sem=sems.at[1, 0], **to("space", above)
        )
        down = pltpu.make_async_remote_copy(
            src_ref=down_src, dst_ref=down_dst, send_sem=sems.at[0, 1], recv_sem=sems.at[1, 1], **to("space", below)
        )
        return [(has_above, has_below, up), (has_below, has_above, down)]

    def start(copies):
        for sends, _, copy in copies:
            pl.when(sends)(copy.start)

    def finish(copies):
        for sends, receives, copy in copies:
            pl.when(sends)(copy.wait_send)
            pl.when(receives)(copy.wait_recv)

    edge_copies = []
    for k, field in enumerate((diff, cour)):
        edge_copies += pair(
            field.at[:, pl.ds(0, 1)],
            field.at[:, pl.ds(rows - 1, 1)],
            edge_recv.at[1, k],
            edge_recv.at[0, k],
            edge_sems.at[k],
        )
    start(edge_copies)
    w_copies = []
    for k, peer in enumerate(tm_peers):
        w_copies.append(
            pltpu.make_async_remote_copy(
                src_ref=weights,
                dst_ref=w_recv.at[section],
                send_sem=w_sems.at[0, k],
                recv_sem=w_sems.at[1, section],
                **to("tm", peer),
            )
        )
    for copy in w_copies:
        copy.start()
    halo_copies = []
    for k, field in enumerate((diff, cour)):
        halo_copies += pair(
            field.at[section, pl.ds(0, halo)],
            field.at[section, pl.ds(rows - halo, halo)],
            halo_recv.at[1, k],
            halo_recv.at[0, k],
            halo_sems.at[k],
        )
    start(halo_copies)

    clear(co_a, co_a.shape[0])
    clear(co_b, co_b.shape[0])
    clear(co_d, co_d.shape[0])

    def put_coefs(row, d, c, inside=None):
        a = 1.0 - 4.0 * d - c
        b = d + c
        if inside is not None:
            a = jnp.where(inside, a, 0.0)
        co_a[row] = a
        co_b[row] = b
        co_d[row] = d

    def adjoint_block(slot, low):
        here = pl.ds(low, BLOCK)
        around = pl.ds(low - 1, BLOCK + 2)
        y = lam[slot, around]
        s = co_d[around] * y
        yc, sc = y[1:-1], s[1:-1]
        return (
            co_a[here] * yc
            + (s[:-2] + s[2:])
            + pltpu.roll(sc, 1, 2)
            + pltpu.roll(co_b[here] * yc, cols - 1, 2)
        )

    def adjoint_step(slot, grown):
        def fn(low):
            lam[1 - slot, pl.ds(low, BLOCK)] = adjoint_block(slot, low)

        over_rows(pad - grown, rows + 2 * grown, fn)

    def add_rows(slot, at, term, count):
        def fn(row, carry):
            lam[slot, at + row] = lam[slot, at + row] + term[row]
            return carry

        lax.fori_loop(0, count, fn, 0)

    def clear_lam():
        clear(lam.at[0], lam.shape[1])
        clear(lam.at[1], lam.shape[1])

    finish(edge_copies)
    reach = steps - 1
    p_copies = []
    for turn in range(n_tm):
        group = lax.rem(section + turn + 1, n_tm)

        def fill(row, carry, group=group):
            put_coefs(pad + row, diff[group, row], cour[group, row])
            return carry

        lax.fori_loop(0, rows, fill, 0)
        put_coefs(pad - 1, edge_recv[0, 0, group, 0], edge_recv[0, 1, group, 0], has_above)
        put_coefs(pad + rows, edge_recv[1, 0, group, 0], edge_recv[1, 1, group, 0], has_below)
        clear_lam()
        slot = 0
        add_rows(slot, pad, forcing.at[group, steps - 1], rows)
        for k in range(1, steps):
            adjoint_step(slot, k)
            slot = 1 - slot
            add_rows(slot, pad, forcing.at[group, steps - 1 - k], rows)
        target = p_send.at[turn] if turn < n_tm - 1 else p_recv.at[section]

        def keep(row, carry, slot=slot, target=target):
            target[row] = lam[slot, pad - reach + row]
            return carry

        lax.fori_loop(0, rows + 2 * reach, keep, 0)
        if turn < n_tm - 1:
            copy = pltpu.make_async_remote_copy(
                src_ref=p_send.at[turn],
                dst_ref=p_recv.at[section],
                send_sem=p_sems.at[0, turn],
                recv_sem=p_sems.at[1, section],
                **to("tm", group),
            )
            copy.start()
            p_copies.append(copy)

    for t in range(total_steps):
        clear(states.at[t], states.shape[1])
        clear(wts.at[t], wts.shape[1])

    def from_peer(k, ref_src, ref_dst, sems):
        peer = tm_peers[k]
        return pltpu.make_async_remote_copy(
            src_ref=ref_src, dst_ref=ref_dst.at[peer], send_sem=sems.at[0, k], recv_sem=sems.at[1, peer], **to("tm", peer)
        )

    for k in range(n_tm - 1):
        w_copies[k].wait_send()
        from_peer(k, weights, w_recv, w_sems).wait_recv()
    w_recv[section] = weights[...]

    def spread_weights(row, carry):
        for t in range(total_steps):
            line = w_recv[t // steps, t % steps, pl.ds(row, 1), :]
            wts[t, pad + row] = jnp.broadcast_to(line, (part, cols))
        return carry

    lax.fori_loop(0, rows, spread_weights, 0)

    finish(halo_copies)

    def fill_halo(row, carry):
        put_coefs(pad - halo + row, halo_recv[0, 0, row], halo_recv[0, 1, row], has_above)
        put_coefs(pad + rows + row, halo_recv[1, 0, row], halo_recv[1, 1, row], has_below)
        return carry

    lax.fori_loop(0, halo, fill_halo, 0)

    for k in range(n_tm - 1):
        p_copies[k].wait_send()
        from_peer(k, p_send.at[k], p_recv, p_sems).wait_recv()
    clear_lam()
    slot = 0
    grown = reach
    add_rows(slot, pad - reach, p_recv.at[n_tm - 1], rows + 2 * reach)
    for other in range(n_tm - 2, -1, -1):
        for _ in range(steps):
            grown += 1
            adjoint_step(slot, grown)
            slot = 1 - slot
        add_rows(slot, pad - reach, p_recv.at[other], rows + 2 * reach)

    def scatter(slot, k):
        copies = pair(lam.at[slot, top], lam.at[slot, bottom], swap_recv.at[k, 1], swap_recv.at[k, 0], swap_sems.at[k])
        start(copies)
        return copies

    def add_scattered(slot, k):
        add_rows(slot, pad, swap_recv.at[k, 0], halo)
        add_rows(slot, pad + rows - halo, swap_recv.at[k, 1], halo)

    def gather(k):
        copies = pair(
            residual.at[pl.ds(0, halo)],
            residual.at[pl.ds(rows - halo, halo)],
            swap_recv.at[k, 1],
            swap_recv.at[k, 0],
            swap_sems.at[k],
        )
        start(copies)
        return copies

    def reduce_over(axis, me, peers, count, tile, k, src, slots, sems):
        src[...] = tile
        slots[me] = tile
        copies = []
        for j, peer in enumerate(peers):
            copies.append(
                pltpu.make_async_remote_copy(
                    src_ref=src,
                    dst_ref=slots.at[me],
                    send_sem=sems.at[0, j],
                    recv_sem=sems.at[1, me],
                    **to(axis, peer),
                )
            )
        for copy in copies:
            copy.start()
        for j, peer in enumerate(peers):
            copies[j].wait_send()
            pltpu.make_async_remote_copy(
                src_ref=src,
                dst_ref=slots.at[peer],
                send_sem=sems.at[0, j],
                recv_sem=sems.at[1, peer],
                **to(axis, peer),
            ).wait_recv()
        total = slots[0]
        for j in range(1, count):
            total = total + slots[j]
        return total

    def reduce_all(partial, k):
        tile = partial[:, :128]
        for piece in range(1, cols // 128):
            tile = tile + partial[:, piece * 128 : (piece + 1) * 128]
        tile = reduce_over("tm", section, tm_peers, n_tm, tile, k, red_src.at[k, 0], red_tm.at[k], red_tm_sems.at[k])
        tile = reduce_over(
            "space", place, space_peers, n_space, tile, k, red_src.at[k, 1], red_space.at[k], red_space_sems.at[k]
        )
        return jnp.sum(jnp.sum(tile, axis=0, keepdims=True), axis=1, keepdims=True)

    none = jnp.zeros((part, cols), F32)
    copies = scatter(slot, 0)
    finish(copies)
    add_scattered(slot, 0)

    def take_rhs(row, acc, slot=slot):
        value = lam[slot, pad + row]
        residual[row] = value
        control[row] = jnp.zeros_like(value)
        return acc + value * value

    partial = lax.fori_loop(0, rows, take_rhs, none)
    swap = 1
    red = 0
    norm_now = None
    for iter_no in range(ITERS):
        copies = gather(swap)
        norm_next = reduce_all(partial, red)
        red += 1
        finish(copies)
        first = iter_no == 0
        beta = None if first else norm_next / norm_now
        norm_now = norm_next

        def new_direction(row, value, beta=beta):
            if beta is not None:
                value = value + beta * direction[row]
            direction[row] = value
            states[0, row] = value
            return value

        def own_direction(row, acc, new=new_direction):
            value = new(pad + row, residual[row])
            return acc + value * value

        def halo_direction(row, carry, new=new_direction, swap=swap):
            new(pad - halo + row, swap_recv[swap, 0, row])
            new(pad + rows + row, swap_recv[swap, 1, row])
            return carry

        squares = lax.fori_loop(0, rows, own_direction, none)
        lax.fori_loop(0, halo, halo_direction, 0)
        swap += 1
        clear_lam()

        def forward_step(t, carry):
            def fn(low):
                here = pl.ds(low, BLOCK)
                x = states[t - 1, pl.ds(low - 1, BLOCK + 2)]
                xc = x[1:-1]
                states[t, here] = (
                    co_a[here] * xc
                    + co_d[here] * (x[:-2] + x[2:] + pltpu.roll(xc, cols - 1, 2))
                    + co_b[here] * pltpu.roll(xc, 1, 2)
                )

            over_rows(pad - halo + t, rows + 2 * (halo - t), fn)
            return carry

        lax.fori_loop(1, total_steps, forward_step, 0)

        def last_term(row, acc):
            x = states[total_steps - 1, pad + row]
            g = wts[total_steps - 1, pad + row] * x
            lam[0, pad + row] = g
            return acc + g * x

        squares = lax.fori_loop(0, rows, last_term, squares)

        def backward_step(k, acc):
            t = total_steps - 2 - k
            slot = lax.rem(k, 2)
            grown = halo - t

            def one(block, acc):
                low = pad - grown + block * BLOCK
                here = pl.ds(low, BLOCK)
                x = states[t, here]
                g = wts[t, here] * x
                lam[1 - slot, here] = adjoint_block(slot, low) + g
                return acc + jnp.sum(g * x, axis=0)

            return lax.fori_loop(0, (rows + 2 * grown + BLOCK - 1) // BLOCK, one, acc)

        squares = lax.fori_loop(0, total_steps - 1, backward_step, squares)
        slot = (total_steps - 1) % 2
        copies = scatter(slot, swap)
        step_len = norm_now / reduce_all(squares, red)
        red += 1
        finish(copies)
        add_scattered(slot, swap)
        swap += 1

        def update(row, acc, slot=slot, step_len=step_len):
            d = direction[pad + row]
            control[row] = control[row] + step_len * d
            value = residual[row] - step_len * (d + lam[slot, pad + row])
            residual[row] = value
            return acc + value * value

        partial = lax.fori_loop(0, rows, update, none)


def solve_call(forcing, weights, diff_t, cour_t, n_space, n_tm):
    sections, steps, rows, part, cols = forcing.shape
    total_steps = steps * n_tm
    halo = total_steps - 1
    ext = rows + 2 * (halo + 1) + BLOCK
    p_rows = rows + 2 * (steps - 1)
    swaps = 1 + 2 * ITERS
    reds = 2 * ITERS
    vmem = pl.BlockSpec(memory_space=pltpu.VMEM)
    row = (part, cols)
    dma = pltpu.SemaphoreType.DMA
    return pl.pallas_call(
        functools.partial(solve_kernel, n_space, n_tm),
        out_shape=[jax.ShapeDtypeStruct((rows, *row), F32)] * 2,
        in_specs=[vmem] * 4,
        out_specs=[vmem] * 2,
        scratch_shapes=[
            pltpu.VMEM((ext, *row), F32),
            pltpu.VMEM((ext, *row), F32),
            pltpu.VMEM((ext, *row), F32),
            pltpu.VMEM((total_steps, ext, *row), F32),
            pltpu.VMEM((total_steps, ext, *row), F32),
            pltpu.VMEM((2, ext, *row), F32),
            pltpu.VMEM((ext, *row), F32),
            pltpu.VMEM((n_tm - 1, p_rows, *row), F32),
            pltpu.VMEM((n_tm, p_rows, *row), F32),
            pltpu.VMEM((n_tm, steps, rows, cols), F32),
            pltpu.VMEM((2, 2, n_tm, 1, *row), F32),
            pltpu.VMEM((2, 2, halo, *row), F32),
            pltpu.VMEM((1, 8, 128), F32),
            pltpu.VMEM((swaps, 2, halo, *row), F32),
            pltpu.VMEM((reds, 2, part, 128), F32),
            pltpu.VMEM((reds, n_tm, part, 128), F32),
            pltpu.VMEM((reds, n_space, part, 128), F32),
            dma((2, n_tm)),
            dma((2, n_tm)),
            dma((2, 2, 2)),
            dma((2, 2, 2)),
            dma((swaps, 2, 2)),
            dma((reds, 2, n_tm)),
            dma((reds, 2, n_space)),
        ],
        compiler_params=pltpu.CompilerParams(
            collective_id=0, has_side_effects=True, vmem_limit_bytes=60 * 2**20
        ),
        name="solve",
    )(forcing, weights, diff_t, cour_t)


def padded_2(cells, sides, width):
    for axis, dim in sides:
        count = lax.axis_size(axis)
        ends = count - 1
        head = lax.slice_in_dim(cells, 0, width, axis=dim)
        tail = lax.slice_in_dim(cells, cells.shape[dim] - width, cells.shape[dim], axis=dim)
        cells = jnp.concatenate(
            [
                lax.ppermute(tail, axis, [(i, (i + 1) % count) for i in range(ends)]),
                cells,
                lax.ppermute(head, axis, [((i + 1) % count, i) for i in range(ends)]),
            ],
            axis=dim,
        )
    return cells


def laplace_rows(padded, state_field):
    return (
        padded[:, 2:, :]
        + padded[:, :-2, :]
        + jnp.roll(state_field, 1, 2)
        + jnp.roll(state_field, -1, 2)
        - 4.0 * state_field
    )


def tangent(state_field, diffusion, courant):
    padded = padded_2(state_field, (("space", 1),), 1)
    return (
        state_field
        + diffusion * laplace_rows(padded, state_field)
        - courant * (state_field - jnp.roll(state_field, 1, 2))
    )


def adjoint(state_field, diffusion, courant):
    carried = courant * state_field
    spread = diffusion * state_field
    padded = padded_2(spread, (("space", 1),), 1)
    return state_field + laplace_rows(padded, spread) - carried + jnp.roll(carried, -1, 2)


def level_squares(residual):
    return lax.psum(jnp.sum(residual * residual), ("space", "tm"))


def level_curve(direction, hessian_image):
    return lax.psum(jnp.sum(direction * hessian_image), ("space", "tm"))


def solve_inner(rhs_field, hessian_part, norm_fn, curve_fn):
    control = jnp.zeros_like(rhs_field)
    residual = rhs_field
    direction = rhs_field
    norm_now = norm_fn(residual)
    for iter_no in range(ITERS):
        hessian_image = direction + hessian_part(direction)
        step_len = norm_now / curve_fn(direction, hessian_image)
        control = control + step_len * direction
        residual = residual - step_len * hessian_image
        if iter_no + 1 < ITERS:
            norm_next = norm_fn(residual)
            direction = residual + norm_next / norm_now * direction
            norm_now = norm_next
    return (control, residual)


def on_device(innovations, obs_counts, diffusion, courant):
    step_dev = obs_counts.shape[0]
    n_sections = lax.axis_size("tm")
    section_pos = lax.axis_index("tm")
    total_steps = step_dev * n_sections
    weights = obs_counts.astype(jnp.float32)[:, None]
    levels, fine_rows, fine_cols = (
        innovations.shape[1],
        innovations.shape[2],
        innovations.shape[3],
    )
    lev_part = levels // n_sections
    rows, cols = fine_rows // COARSE, fine_cols // COARSE
    if lev_part == 8 and rows % 8 == 0 and rows >= total_steps - 1 and cols % 128 == 0:
        forced = restrict_call(innovations, obs_counts, diffusion, courant, n_sections)
        solved = solve_call(*forced, lax.axis_size("space"), n_sections)
        return tuple(expand_call(*solved))
    blocks = innovations.reshape(step_dev, levels, fine_rows // 4, 4, fine_cols // 4, 4).astype(
        jnp.float32
    )
    forcing = weights * jnp.mean(blocks, axis=(3, 5))
    all_weights = lax.all_gather(obs_counts, "tm", axis=0, tiled=True).astype(jnp.float32)[:, None]
    all_forcing = lax.all_to_all(forcing, "tm", split_axis=1, concat_axis=0, tiled=True)
    diff_part = lax.dynamic_slice_in_dim(diffusion, section_pos * lev_part, lev_part, 0)
    cour_part = lax.dynamic_slice_in_dim(courant, section_pos * lev_part, lev_part, 0)

    def level_back(terms):
        current = terms[total_steps - 1]
        for step_no in range(total_steps - 2, -1, -1):
            current = terms[step_no] + adjoint(current, diff_part, cour_part)
        return current

    def level_hess(state_field):
        records = []
        for step_no in range(total_steps):
            records.append(all_weights[step_no] * state_field)
            if step_no + 1 < total_steps:
                state_field = tangent(state_field, diff_part, cour_part)
        return level_back(jnp.stack(records))

    control, residual = solve_inner(level_back(all_forcing), level_hess, level_squares, level_curve)
    increment = jnp.repeat(jnp.repeat(control, 4, axis=1), 4, axis=2)
    return (increment, residual)


def solution(mesh):
    placed = (
        P("tm", None, "space", None),
        P("tm", "space", None),
        P(None, "space", None),
        P(None, "space", None),
    )
    return jax.shard_map(
        on_device,
        mesh=mesh,
        in_specs=placed,
        out_specs=(P("tm", "space", None), P("tm", "space", None)),
        check_vma=False,
    )
```

```python
import functools

import jax
import jax.numpy as jnp
from jax import lax
from jax.experimental import pallas as pl
from jax.experimental.pallas import tpu as pltpu
from jax.sharding import PartitionSpec as P

ITERS = 3
F32 = jnp.float32
BF16 = jnp.bfloat16
MESH = pl.DeviceIdType.MESH
BLOCK = 4
ROWS = 4
COARSE = 4


def restrict_kernel(inn, counts, diff, cour, forcing, weights, diff_t, cour_t, summed, turned):
    levels, fine_rows, fine_cols = inn.shape[1:]
    rows, cols = fine_rows // COARSE, fine_cols // COARSE
    weights[0] = counts[0].astype(F32)
    wide = 128 * COARSE
    pick = jnp.where(
        lax.broadcasted_iota(jnp.int32, (wide, 128), 0) // COARSE
        == lax.broadcasted_iota(jnp.int32, (wide, 128), 1),
        1.0 / (COARSE * COARSE),
        0.0,
    ).astype(BF16)
    for part in range(cols // 128):
        block = inn[0, :, :, part * wide : (part + 1) * wide].reshape(levels * fine_rows, wide)
        summed[part] = jnp.dot(block, pick, preferred_element_type=F32)
    for part in range(cols // 128):
        at = slice(part * 128, (part + 1) * 128)
        scale = weights[0, :, at]
        for level in range(levels):
            total = summed[part, pl.ds(level * fine_rows, rows, stride=COARSE), :]
            for sub in range(1, COARSE):
                total += summed[part, pl.ds(level * fine_rows + sub, rows, stride=COARSE), :]
            turned[part, pl.ds(level, rows, stride=levels), :] = total * scale
        forcing[0, 0, :, :, at] = turned[part].reshape(rows, levels, 128)

    @pl.when(pl.program_id(1) == 0)
    def _():
        for row in range(rows):
            diff_t[0, row] = diff[:, row, :]
            cour_t[0, row] = cour[:, row, :]


def restrict_call(innovations, obs_counts, diffusion, courant, sections):
    steps, levels, fine_rows, fine_cols = innovations.shape
    part = levels // sections
    rows, cols = fine_rows // COARSE, fine_cols // COARSE
    field = pl.BlockSpec((part, rows, cols), lambda g, t: (g, 0, 0))
    field_t = pl.BlockSpec((1, rows, part, cols), lambda g, t: (g, 0, 0, 0))
    step = pl.BlockSpec((1, rows, cols), lambda g, t: (t, 0, 0))
    return pl.pallas_call(
        restrict_kernel,
        grid=(sections, steps),
        in_specs=[
            pl.BlockSpec((1, part, fine_rows, fine_cols), lambda g, t: (t, g, 0, 0)),
            step,
            field,
            field,
        ],
        out_specs=[
            pl.BlockSpec((1, 1, rows, part, cols), lambda g, t: (g, t, 0, 0, 0)),
            step,
            field_t,
            field_t,
        ],
        out_shape=[
            jax.ShapeDtypeStruct((sections, steps, rows, part, cols), F32),
            jax.ShapeDtypeStruct((steps, rows, cols), F32),
            jax.ShapeDtypeStruct((sections, rows, part, cols), F32),
            jax.ShapeDtypeStruct((sections, rows, part, cols), F32),
        ],
        scratch_shapes=[
            pltpu.VMEM((cols // 128, part * fine_rows, 128), F32),
            pltpu.VMEM((cols // 128, part * rows, 128), F32),
        ],
        compiler_params=pltpu.CompilerParams(vmem_limit_bytes=48 * 2**20),
        name="restrict",
    )(innovations, obs_counts, diffusion, courant)


def expand_kernel(control, residual, increment, residual_out, held, repeated):
    rows, cols = residual_out.shape[1:]
    part = control.shape[0] // rows
    level = pl.program_id(0)
    wide = 128 * COARSE

    @pl.when(level == 0)
    def _():
        for piece in range(cols // 128):
            held[0, piece] = control[:, piece * 128 : (piece + 1) * 128]
            held[1, piece] = residual[:, piece * 128 : (piece + 1) * 128]

    pick = jnp.where(
        lax.broadcasted_iota(jnp.int32, (128, wide), 1) // COARSE
        == lax.broadcasted_iota(jnp.int32, (128, wide), 0),
        1.0,
        0.0,
    ).astype(BF16)
    for piece in range(cols // 128):
        at = pl.ds(level, rows, stride=part)
        residual_out[0, :, piece * 128 : (piece + 1) * 128] = held[1, piece, at, :]
        values = held[0, piece, at, :]
        for sub in range(COARSE):
            repeated[piece, pl.ds(sub, rows, stride=COARSE), :] = values
        rest = repeated[piece]
        total = None
        for _ in range(3):
            head = rest.astype(BF16)
            rest = rest - head.astype(F32)
            spread = jnp.dot(head, pick, preferred_element_type=F32)
            total = spread if total is None else total + spread
        increment[0, :, piece * wide : (piece + 1) * wide] = total


def expand_call(control, residual):
    rows, part, cols = control.shape
    whole = pl.BlockSpec((rows * part, cols), lambda l: (0, 0))
    return pl.pallas_call(
        expand_kernel,
        grid=(part,),
        in_specs=[whole, whole],
        out_specs=[
            pl.BlockSpec((1, rows * COARSE, cols * COARSE), lambda l: (l, 0, 0)),
            pl.BlockSpec((1, rows, cols), lambda l: (l, 0, 0)),
        ],
        out_shape=[
            jax.ShapeDtypeStruct((part, rows * COARSE, cols * COARSE), F32),
            jax.ShapeDtypeStruct((part, rows, cols), F32),
        ],
        scratch_shapes=[
            pltpu.VMEM((2, cols // 128, rows * part, 128), F32),
            pltpu.VMEM((cols // 128, rows * COARSE, 128), F32),
        ],
        compiler_params=pltpu.CompilerParams(vmem_limit_bytes=32 * 2**20),
        name="expand",
    )(control.reshape(rows * part, cols), residual.reshape(rows * part, cols))


def solve_kernel(
    n_space,
    n_tm,
    forcing,
    weights,
    diff,
    cour,
    control,
    residual,
    co_a,
    co_b,
    co_d,
    states,
    wts,
    lam,
    direction,
    p_send,
    p_recv,
    w_recv,
    edge_recv,
    halo_recv,
    send_buf,
    swap_recv,
    red_src,
    red_tm,
    red_space,
    p_sems,
    w_sems,
    edge_sems,
    halo_sems,
    swap_sems,
    red_tm_sems,
    red_space_sems,
):
    steps, rows, part, cols = forcing.shape[1:]
    total_steps = steps * n_tm
    halo = total_steps - 1
    pad = halo + 1
    place = lax.axis_index("space")
    section = lax.axis_index("tm")
    above, below = place - 1, place + 1
    has_above, has_below = place > 0, place < n_space - 1
    own = pl.ds(pad, rows)
    top, bottom = pl.ds(pad - halo, halo), pl.ds(pad + rows, halo)

    def over_rows(low, count, fn):
        blocks = (count + BLOCK - 1) // BLOCK

        def one(block, carry):
            fn(low + block * BLOCK)
            return carry

        lax.fori_loop(0, blocks, one, 0)

    def by_block(count, fn, carry=0):
        full = count // ROWS

        def one(block, carry):
            return fn(block * ROWS, ROWS, carry)

        if full:
            carry = lax.fori_loop(0, full, one, carry)
        if count % ROWS:
            carry = fn(full * ROWS, count % ROWS, carry)
        return carry

    def clear(ref, count, first=0):
        def one(row, size, carry):
            ref[pl.ds(first + row, size)] = jnp.zeros((size, *ref.shape[1:]), F32)
            return carry

        by_block(count, one)

    def to(axis, peer):
        return {"device_id": {axis: peer}, "device_id_type": MESH}

    edge_recv[...] = jnp.zeros_like(edge_recv)
    for side in range(2):
        for k in range(2):
            clear(halo_recv.at[side, k], halo)
        for k in range(swap_recv.shape[0]):
            clear(swap_recv.at[k, side], halo)

    tm_peers = [lax.rem(section + k, n_tm) for k in range(1, n_tm)]
    space_peers = [lax.rem(place + k, n_space) for k in range(1, n_space)]
    barrier = pltpu.get_barrier_semaphore()
    for peer in tm_peers:
        pl.semaphore_signal(barrier, inc=1, **to("tm", peer))
    for peer in space_peers:
        pl.semaphore_signal(barrier, inc=1, **to("space", peer))
    pl.semaphore_wait(barrier, n_tm - 1 + n_space - 1)

    def pair(up_src, down_src, up_dst, down_dst, sems):
        up = pltpu.make_async_remote_copy(
            src_ref=up_src, dst_ref=up_dst, send_sem=sems.at[0, 0], recv_sem=sems.at[1, 0], **to("space", above)
        )
        down = pltpu.make_async_remote_copy(
            src_ref=down_src, dst_ref=down_dst, send_sem=sems.at[0, 1], recv_sem=sems.at[1, 1], **to("space", below)
        )
        return [(has_above, has_below, up), (has_below, has_above, down)]

    def start(copies):
        for sends, _, copy in copies:
            pl.when(sends)(copy.start)

    def finish(copies):
        for sends, receives, copy in copies:
            pl.when(sends)(copy.wait_send)
            pl.when(receives)(copy.wait_recv)

    edge_copies = []
    for k, field in enumerate((diff, cour)):
        edge_copies += pair(
            field.at[:, pl.ds(0, 1)],
            field.at[:, pl.ds(rows - 1, 1)],
            edge_recv.at[1, k],
            edge_recv.at[0, k],
            edge_sems.at[k],
        )
    start(edge_copies)
    w_copies = []
    for k, peer in enumerate(tm_peers):
        w_copies.append(
            pltpu.make_async_remote_copy(
                src_ref=weights,
                dst_ref=w_recv.at[section],
                send_sem=w_sems.at[0, k],
                recv_sem=w_sems.at[1, section],
                **to("tm", peer),
            )
        )
    for copy in w_copies:
        copy.start()
    halo_copies = []
    for k, field in enumerate((diff, cour)):
        halo_copies += pair(
            field.at[section, pl.ds(0, halo)],
            field.at[section, pl.ds(rows - halo, halo)],
            halo_recv.at[1, k],
            halo_recv.at[0, k],
            halo_sems.at[k],
        )
    start(halo_copies)

    clear(co_a, co_a.shape[0])
    clear(co_b, co_b.shape[0])
    clear(co_d, co_d.shape[0])

    def put_coefs(row, d, c, inside=None):
        a = 1.0 - 4.0 * d - c
        b = d + c
        if inside is not None:
            a = jnp.where(inside, a, 0.0)
        co_a[row] = a
        co_b[row] = b
        co_d[row] = d

    def adjoint_block(slot, low):
        here = pl.ds(low, BLOCK)
        around = pl.ds(low - 1, BLOCK + 2)
        y = lam[slot, around]
        s = co_d[around] * y
        yc, sc = y[1:-1], s[1:-1]
        return (
            co_a[here] * yc
            + (s[:-2] + s[2:])
            + pltpu.roll(sc, 1, 2)
            + pltpu.roll(co_b[here] * yc, cols - 1, 2)
        )

    def adjoint_step(slot, grown):
        def fn(low):
            lam[1 - slot, pl.ds(low, BLOCK)] = adjoint_block(slot, low)

        over_rows(pad - grown, rows + 2 * grown, fn)

    def add_rows(slot, at, term, count):
        def fn(row, size, carry):
            here = pl.ds(at + row, size)
            lam[slot, here] = lam[slot, here] + term[pl.ds(row, size)]
            return carry

        by_block(count, fn)

    def clear_lam():
        clear(lam.at[0], lam.shape[1])
        clear(lam.at[1], lam.shape[1])

    finish(edge_copies)
    reach = steps - 1
    p_copies = []
    for turn in range(n_tm):
        group = lax.rem(section + turn + 1, n_tm)

        def fill(row, size, carry, group=group):
            here = pl.ds(row, size)
            put_coefs(pl.ds(pad + row, size), diff[group, here], cour[group, here])
            return carry

        by_block(rows, fill)
        put_coefs(pad - 1, edge_recv[0, 0, group, 0], edge_recv[0, 1, group, 0], has_above)
        put_coefs(pad + rows, edge_recv[1, 0, group, 0], edge_recv[1, 1, group, 0], has_below)
        clear_lam()
        slot = 0
        add_rows(slot, pad, forcing.at[group, steps - 1], rows)
        for k in range(1, steps):
            adjoint_step(slot, k)
            slot = 1 - slot
            add_rows(slot, pad, forcing.at[group, steps - 1 - k], rows)
        target = p_send.at[turn] if turn < n_tm - 1 else p_recv.at[section]

        def keep(row, size, carry, slot=slot, target=target):
            target[pl.ds(row, size)] = lam[slot, pl.ds(pad - reach + row, size)]
            return carry

        by_block(rows + 2 * reach, keep)
        if turn < n_tm - 1:
            copy = pltpu.make_async_remote_copy(
                src_ref=p_send.at[turn],
                dst_ref=p_recv.at[section],
                send_sem=p_sems.at[0, turn],
                recv_sem=p_sems.at[1, section],
                **to("tm", group),
            )
            copy.start()
            p_copies.append(copy)

    for t in range(total_steps):
        clear(states.at[t], states.shape[1] - pad - rows, pad + rows)
        clear(wts.at[t], pad)
        clear(wts.at[t], wts.shape[1] - pad - rows, pad + rows)

    def from_peer(k, ref_src, ref_dst, sems):
        peer = tm_peers[k]
        return pltpu.make_async_remote_copy(
            src_ref=ref_src, dst_ref=ref_dst.at[peer], send_sem=sems.at[0, k], recv_sem=sems.at[1, peer], **to("tm", peer)
        )

    for k in range(n_tm - 1):
        w_copies[k].wait_send()
        from_peer(k, weights, w_recv, w_sems).wait_recv()
    w_recv[section] = weights[...]

    def spread_weights(row, carry):
        for t in range(total_steps):
            line = w_recv[t // steps, t % steps, pl.ds(row, 1), :]
            wts[t, pad + row] = jnp.broadcast_to(line, (part, cols))
        return carry

    lax.fori_loop(0, rows, spread_weights, 0)

    finish(halo_copies)

    def fill_halo(row, size, carry):
        here = pl.ds(row, size)
        put_coefs(pl.ds(pad - halo + row, size), halo_recv[0, 0, here], halo_recv[0, 1, here], has_above)
        put_coefs(pl.ds(pad + rows + row, size), halo_recv[1, 0, here], halo_recv[1, 1, here], has_below)
        return carry

    by_block(halo, fill_halo)

    for k in range(n_tm - 1):
        p_copies[k].wait_send()
        from_peer(k, p_send.at[k], p_recv, p_sems).wait_recv()
    clear_lam()
    slot = 0
    grown = reach
    add_rows(slot, pad - reach, p_recv.at[n_tm - 1], rows + 2 * reach)
    for other in range(n_tm - 2, -1, -1):
        for _ in range(steps):
            grown += 1
            adjoint_step(slot, grown)
            slot = 1 - slot
        add_rows(slot, pad - reach, p_recv.at[other], rows + 2 * reach)

    def scatter(slot, k):
        copies = pair(lam.at[slot, top], lam.at[slot, bottom], swap_recv.at[k, 1], swap_recv.at[k, 0], swap_sems.at[k])
        start(copies)
        return copies

    def add_scattered(slot, k):
        add_rows(slot, pad, swap_recv.at[k, 0], halo)
        add_rows(slot, pad + rows - halo, swap_recv.at[k, 1], halo)

    def gather(k):
        copies = pair(
            residual.at[pl.ds(0, halo)],
            residual.at[pl.ds(rows - halo, halo)],
            swap_recv.at[k, 1],
            swap_recv.at[k, 0],
            swap_sems.at[k],
        )
        start(copies)
        return copies

    def reduce_over(axis, me, peers, count, tile, k, src, slots, sems):
        src[...] = tile
        slots[me] = tile
        copies = []
        for j, peer in enumerate(peers):
            copies.append(
                pltpu.make_async_remote_copy(
                    src_ref=src,
                    dst_ref=slots.at[me],
                    send_sem=sems.at[0, j],
                    recv_sem=sems.at[1, me],
                    **to(axis, peer),
                )
            )
        for copy in copies:
            copy.start()
        for j, peer in enumerate(peers):
            copies[j].wait_send()
            pltpu.make_async_remote_copy(
                src_ref=src,
                dst_ref=slots.at[peer],
                send_sem=sems.at[0, j],
                recv_sem=sems.at[1, peer],
                **to(axis, peer),
            ).wait_recv()
        total = slots[0]
        for j in range(1, count):
            total = total + slots[j]
        return total

    def reduce_all(partial, k):
        tile = partial[:, :128]
        for piece in range(1, cols // 128):
            tile = tile + partial[:, piece * 128 : (piece + 1) * 128]
        tile = reduce_over("tm", section, tm_peers, n_tm, tile, k, red_src.at[k, 0], red_tm.at[k], red_tm_sems.at[k])
        tile = reduce_over(
            "space", place, space_peers, n_space, tile, k, red_src.at[k, 1], red_space.at[k], red_space_sems.at[k]
        )
        return jnp.sum(jnp.sum(tile, axis=0, keepdims=True), axis=1, keepdims=True)

    none = jnp.zeros((part, cols), F32)
    copies = scatter(slot, 0)
    finish(copies)
    add_scattered(slot, 0)

    def take_rhs(row, size, acc, slot=slot):
        value = lam[slot, pl.ds(pad + row, size)]
        residual[pl.ds(row, size)] = value
        control[pl.ds(row, size)] = jnp.zeros_like(value)
        return acc + jnp.sum(value * value, axis=0)

    partial = by_block(rows, take_rhs, none)
    swap = 1
    red = 0
    norm_now = None
    for iter_no in range(ITERS):
        copies = gather(swap)
        norm_next = reduce_all(partial, red)
        red += 1
        finish(copies)
        first = iter_no == 0
        beta = None if first else norm_next / norm_now
        norm_now = norm_next

        def new_direction(here, value, beta=beta):
            if beta is not None:
                value = value + beta.reshape(1, 1, 1) * direction[here]
            direction[here] = value
            states[0, here] = value
            return value

        def own_direction(row, size, acc, new=new_direction):
            value = new(pl.ds(pad + row, size), residual[pl.ds(row, size)])
            return acc + jnp.sum(value * value, axis=0)

        def halo_direction(row, size, carry, new=new_direction, swap=swap):
            here = pl.ds(row, size)
            new(pl.ds(pad - halo + row, size), swap_recv[swap, 0, here])
            new(pl.ds(pad + rows + row, size), swap_recv[swap, 1, here])
            return carry

        squares = by_block(rows, own_direction, none)
        by_block(halo, halo_direction)
        swap += 1
        clear_lam()

        def forward_step(t, carry):
            def fn(low):
                here = pl.ds(low, BLOCK)
                x = states[t - 1, pl.ds(low - 1, BLOCK + 2)]
                xc = x[1:-1]
                states[t, here] = (
                    co_a[here] * xc
                    + co_d[here] * (x[:-2] + x[2:] + pltpu.roll(xc, cols - 1, 2))
                    + co_b[here] * pltpu.roll(xc, 1, 2)
                )

            over_rows(pad - halo + t, rows + 2 * (halo - t), fn)
            return carry

        lax.fori_loop(1, total_steps, forward_step, 0)

        def last_term(row, size, acc):
            here = pl.ds(pad + row, size)
            x = states[total_steps - 1, here]
            g = wts[total_steps - 1, here] * x
            lam[0, here] = g
            return acc + jnp.sum(g * x, axis=0)

        squares = by_block(rows, last_term, squares)

        def backward_step(k, acc):
            t = total_steps - 2 - k
            slot = lax.rem(k, 2)
            grown = halo - t

            def one(block, acc):
                low = pad - grown + block * BLOCK
                here = pl.ds(low, BLOCK)
                x = states[t, here]
                g = wts[t, here] * x
                lam[1 - slot, here] = adjoint_block(slot, low) + g
                return acc + jnp.sum(g * x, axis=0)

            return lax.fori_loop(0, (rows + 2 * grown + BLOCK - 1) // BLOCK, one, acc)

        squares = lax.fori_loop(0, total_steps - 1, backward_step, squares)
        slot = (total_steps - 1) % 2
        copies = scatter(slot, swap)
        step_len = norm_now / reduce_all(squares, red)
        red += 1
        finish(copies)
        add_scattered(slot, swap)
        swap += 1

        def update(row, size, acc, slot=slot, step_len=step_len.reshape(1, 1, 1)):
            here, ext = pl.ds(row, size), pl.ds(pad + row, size)
            d = direction[ext]
            control[here] = control[here] + step_len * d
            value = residual[here] - step_len * (d + lam[slot, ext])
            residual[here] = value
            return acc + jnp.sum(value * value, axis=0)

        partial = by_block(rows, update, none)


def solve_call(forcing, weights, diff_t, cour_t, n_space, n_tm):
    sections, steps, rows, part, cols = forcing.shape
    total_steps = steps * n_tm
    halo = total_steps - 1
    ext = rows + 2 * (halo + 1) + BLOCK
    p_rows = rows + 2 * (steps - 1)
    swaps = 1 + 2 * ITERS
    reds = 2 * ITERS
    vmem = pl.BlockSpec(memory_space=pltpu.VMEM)
    row = (part, cols)
    dma = pltpu.SemaphoreType.DMA
    return pl.pallas_call(
        functools.partial(solve_kernel, n_space, n_tm),
        out_shape=[jax.ShapeDtypeStruct((rows, *row), F32)] * 2,
        in_specs=[vmem] * 4,
        out_specs=[vmem] * 2,
        scratch_shapes=[
            pltpu.VMEM((ext, *row), F32),
            pltpu.VMEM((ext, *row), F32),
            pltpu.VMEM((ext, *row), F32),
            pltpu.VMEM((total_steps, ext, *row), F32),
            pltpu.VMEM((total_steps, ext, *row), F32),
            pltpu.VMEM((2, ext, *row), F32),
            pltpu.VMEM((ext, *row), F32),
            pltpu.VMEM((n_tm - 1, p_rows, *row), F32),
            pltpu.VMEM((n_tm, p_rows, *row), F32),
            pltpu.VMEM((n_tm, steps, rows, cols), F32),
            pltpu.VMEM((2, 2, n_tm, 1, *row), F32),
            pltpu.VMEM((2, 2, halo, *row), F32),
            pltpu.VMEM((1, 8, 128), F32),
            pltpu.VMEM((swaps, 2, halo, *row), F32),
            pltpu.VMEM((reds, 2, part, 128), F32),
            pltpu.VMEM((reds, n_tm, part, 128), F32),
            pltpu.VMEM((reds, n_space, part, 128), F32),
            dma((2, n_tm)),
            dma((2, n_tm)),
            dma((2, 2, 2)),
            dma((2, 2, 2)),
            dma((swaps, 2, 2)),
            dma((reds, 2, n_tm)),
            dma((reds, 2, n_space)),
        ],
        compiler_params=pltpu.CompilerParams(
            collective_id=0, has_side_effects=True, vmem_limit_bytes=60 * 2**20
        ),
        name="solve",
    )(forcing, weights, diff_t, cour_t)


def padded_2(cells, sides, width):
    for axis, dim in sides:
        count = lax.axis_size(axis)
        ends = count - 1
        head = lax.slice_in_dim(cells, 0, width, axis=dim)
        tail = lax.slice_in_dim(cells, cells.shape[dim] - width, cells.shape[dim], axis=dim)
        cells = jnp.concatenate(
            [
                lax.ppermute(tail, axis, [(i, (i + 1) % count) for i in range(ends)]),
                cells,
                lax.ppermute(head, axis, [((i + 1) % count, i) for i in range(ends)]),
            ],
            axis=dim,
        )
    return cells


def laplace_rows(padded, state_field):
    return (
        padded[:, 2:, :]
        + padded[:, :-2, :]
        + jnp.roll(state_field, 1, 2)
        + jnp.roll(state_field, -1, 2)
        - 4.0 * state_field
    )


def tangent(state_field, diffusion, courant):
    padded = padded_2(state_field, (("space", 1),), 1)
    return (
        state_field
        + diffusion * laplace_rows(padded, state_field)
        - courant * (state_field - jnp.roll(state_field, 1, 2))
    )


def adjoint(state_field, diffusion, courant):
    carried = courant * state_field
    spread = diffusion * state_field
    padded = padded_2(spread, (("space", 1),), 1)
    return state_field + laplace_rows(padded, spread) - carried + jnp.roll(carried, -1, 2)


def level_squares(residual):
    return lax.psum(jnp.sum(residual * residual), ("space", "tm"))


def level_curve(direction, hessian_image):
    return lax.psum(jnp.sum(direction * hessian_image), ("space", "tm"))


def solve_inner(rhs_field, hessian_part, norm_fn, curve_fn):
    control = jnp.zeros_like(rhs_field)
    residual = rhs_field
    direction = rhs_field
    norm_now = norm_fn(residual)
    for iter_no in range(ITERS):
        hessian_image = direction + hessian_part(direction)
        step_len = norm_now / curve_fn(direction, hessian_image)
        control = control + step_len * direction
        residual = residual - step_len * hessian_image
        if iter_no + 1 < ITERS:
            norm_next = norm_fn(residual)
            direction = residual + norm_next / norm_now * direction
            norm_now = norm_next
    return (control, residual)


def on_device(innovations, obs_counts, diffusion, courant):
    step_dev = obs_counts.shape[0]
    n_sections = lax.axis_size("tm")
    section_pos = lax.axis_index("tm")
    total_steps = step_dev * n_sections
    weights = obs_counts.astype(jnp.float32)[:, None]
    levels, fine_rows, fine_cols = (
        innovations.shape[1],
        innovations.shape[2],
        innovations.shape[3],
    )
    lev_part = levels // n_sections
    rows, cols = fine_rows // COARSE, fine_cols // COARSE
    if lev_part == 8 and rows % 8 == 0 and rows >= total_steps - 1 and cols % 128 == 0:
        forced = restrict_call(innovations, obs_counts, diffusion, courant, n_sections)
        solved = solve_call(*forced, lax.axis_size("space"), n_sections)
        return tuple(expand_call(*solved))
    blocks = innovations.reshape(step_dev, levels, fine_rows // 4, 4, fine_cols // 4, 4).astype(
        jnp.float32
    )
    forcing = weights * jnp.mean(blocks, axis=(3, 5))
    all_weights = lax.all_gather(obs_counts, "tm", axis=0, tiled=True).astype(jnp.float32)[:, None]
    all_forcing = lax.all_to_all(forcing, "tm", split_axis=1, concat_axis=0, tiled=True)
    diff_part = lax.dynamic_slice_in_dim(diffusion, section_pos * lev_part, lev_part, 0)
    cour_part = lax.dynamic_slice_in_dim(courant, section_pos * lev_part, lev_part, 0)

    def level_back(terms):
        current = terms[total_steps - 1]
        for step_no in range(total_steps - 2, -1, -1):
            current = terms[step_no] + adjoint(current, diff_part, cour_part)
        return current

    def level_hess(state_field):
        records = []
        for step_no in range(total_steps):
            records.append(all_weights[step_no] * state_field)
            if step_no + 1 < total_steps:
                state_field = tangent(state_field, diff_part, cour_part)
        return level_back(jnp.stack(records))

    control, residual = solve_inner(level_back(all_forcing), level_hess, level_squares, level_curve)
    increment = jnp.repeat(jnp.repeat(control, 4, axis=1), 4, axis=2)
    return (increment, residual)


def solution(mesh):
    placed = (
        P("tm", None, "space", None),
        P("tm", "space", None),
        P(None, "space", None),
        P(None, "space", None),
    )
    return jax.shard_map(
        on_device,
        mesh=mesh,
        in_specs=placed,
        out_specs=(P("tm", "space", None), P("tm", "space", None)),
        check_vma=False,
    )
```
